32 devices in a mesh: row: 16 (over z, y, x), col: 2 (over core).
Axes of the slice: x: 2, y: 2, z: 4, core: 2. Of those that a mesh axis runs over, the one named last changes fastest.
Arguments:
- sources: bfloat16 [32768, 640], P(('row', 'col')), may hold values from -6 to 6
- tree_perm: int32 [32768], P(('row', 'col')), may hold values from 0 to 32767, as said below
- leaf_blocks: bfloat16 [32768, 512], P(('row', 'col')), may hold values from -0.25 to 0.25
- u_factors: bfloat16 [6, 32, 32768], P(None, None, ('row', 'col')), may hold values from -0.4375 to 0.4375
- v_factors: bfloat16 [6, 32, 32768], P(None, None, ('row', 'col')), as said below
- level_ranks: int32 [6], replicated, may hold values from 16 to 32
Outputs:
- products: bfloat16 [32768, 640], P(('row', 'col'))
The draws below stay inside these ranges and needn't reach their ends.
Inputs may be any that keep to these rules, and one draw needn't show every extreme that they name: tree_perm is a permutation that maps each aligned block of 1024 positions onto the same block of initial indices. `v_factors`: entries of level l are of the order of the inverse square root of 32768 / 2^l.
All inputs are finite; a program needn't handle non-finite values.
Results may differ from the reference program's by a relative error of at most 0.0037.
Values sent between devices are 32-bit elements; how exact they have to be, the bound alone decides.
A program may use at most 64 MiB of HBM per device.

```python
import jax
import jax.numpy as jnp
from jax import lax

LEAF = 512
K = 32
RHS = 640
ROWS_DEV = 1024
N = 32768
LEVELS = 6


def draw_tree_perm(key, part):
    blocks = N // ROWS_DEV
    keys = jax.random.split(key, blocks)
    perms = jax.vmap(lambda one_key: jax.random.permutation(one_key, ROWS_DEV))(keys).astype(jnp.int32)
    offsets = jnp.arange(blocks, dtype=jnp.int32)[:, None] * ROWS_DEV
    return (perms + offsets).reshape(N).astype(jnp.int32)


def draw_v_factors(key, part):
    level_scale = jnp.sqrt(2.0 ** (jnp.arange(LEVELS, dtype=jnp.float32) + 1.0) / N)
    base = jax.random.normal(key, (LEVELS, K, N), jnp.float32)
    return (base * level_scale[:, None, None]).astype(jnp.bfloat16)


def set_ends(array, stream_key, low, top_value):
    shape = array.shape
    place = [jax.random.randint(jax.random.fold_in(stream_key, axis), (), 0, shape[axis]) for axis in range(len(shape))]
    array = array.at[tuple(place)].set(low)
    longest = shape.index(max(shape))
    place[longest] = (place[longest] + 1) % shape[longest]
    return array.at[tuple(place)].set(top_value)


def levels(rng, extent, cuts, smallest, largest):
    level = 1.0
    for dim, blocks in cuts:
        steps = jax.random.uniform(jax.random.fold_in(jax.random.fold_in(rng, 6), dim), (blocks,), jnp.float32, smallest / len(cuts), largest / len(cuts))
        level = level * jnp.repeat(jnp.exp(steps), extent[dim] // blocks).reshape((-1,) + (1,) * (len(extent) - 1 - dim))
    return level


def bell_draw(stream_key, shape, width, most, cuts=(), held_as=jnp.bfloat16):
    array = width * jax.random.normal(stream_key, shape, jnp.float32)
    if cuts:
        array = array * levels(stream_key, shape, cuts, -0.22, 0.18)
    return jnp.clip(array, -most, most).astype(held_as)


def setup_inputs(seed: int = 0) -> dict:
    arg_keys = jax.random.split(jax.random.key(seed), 7)
    return {
        "sources": bell_draw(arg_keys[0], (N, RHS), 1.0, 6.0, ((0, 32),)),
        "tree_perm": draw_tree_perm(jax.random.fold_in(arg_keys[6], 71), 0),
        "leaf_blocks": bell_draw(arg_keys[2], (N, LEAF), LEAF ** -0.5, 0.25, ((0, 32),)),
        "u_factors": bell_draw(arg_keys[3], (LEVELS, K, N), (K * LEVELS) ** -0.5, 0.4375, ((2, 32),)),
        "v_factors": draw_v_factors(jax.random.fold_in(arg_keys[6], 71), 0),
        "level_ranks": set_ends(jax.random.randint(arg_keys[5], (LEVELS,), K // 2, K + 1), jax.random.fold_in(arg_keys[5], 1), K // 2, K).astype(jnp.int32),
    }


def reference(sources, tree_perm, leaf_blocks, u_factors, v_factors, level_ranks):
    ordered = sources[tree_perm].astype(jnp.float32)
    leaf_count = N // LEAF
    result = jnp.einsum("gij,gjr->gir", leaf_blocks.reshape(leaf_count, LEAF, LEAF).astype(jnp.float32), ordered.reshape(leaf_count, LEAF, RHS)).reshape(N, RHS)
    rank_index = lax.iota(jnp.int32, K)
    for level in range(LEVELS):
        groups = 2 ** (level + 1)
        cluster_rows = N // groups
        v_level = v_factors[level].astype(jnp.float32).reshape(K, groups, cluster_rows)
        coef = jnp.einsum("kgs,gsr->gkr", v_level, ordered.reshape(groups, cluster_rows, RHS))
        far_coef = coef.reshape(groups // 2, 2, K, RHS)[:, ::-1].reshape(groups, K, RHS)
        rank_mask = (rank_index < level_ranks[level]).astype(jnp.float32)
        far_coef = (far_coef * rank_mask[None, :, None]).astype(jnp.bfloat16).astype(jnp.float32)
        u_level = u_factors[level].astype(jnp.float32).reshape(K, groups, cluster_rows)
        result = result + jnp.einsum("kgs,gkr->gsr", u_level, far_coef).reshape(N, RHS)
    tree_out = result.astype(jnp.bfloat16)
    return jnp.zeros((N, RHS), jnp.bfloat16).at[tree_perm].set(tree_out)
```

```python
import functools

import jax
import jax.numpy as jnp
from jax import lax
from jax.experimental import pallas as pl
from jax.experimental.pallas import tpu as pltpu
from jax.sharding import PartitionSpec as P

F32 = jnp.float32
BF16 = jnp.bfloat16


def flip(x, mask):
    bit = 0
    while mask >> bit:
        if mask >> bit & 1:
            x = x + (1 << bit) * (1 - 2 * lax.rem(lax.div(x, 1 << bit), 2))
        bit += 1
    return x


def split_bits(dev_bits):
    groups, start = [], 0
    while start < dev_bits:
        bits = min(3, dev_bits - start)
        groups.append((start, bits))
        start += bits
    return groups


def top_bit(k):
    return k.bit_length() - 1


def kernel(
    cfg,
    ranks_ref, perm_ref, src_hbm, leaf_hbm, u_hbm, v_hbm,
    out_hbm,
    src, leaf, u, v, one_hot, one_hot_t, ordered, mixed, u_perm, u_near, near, acc, far, staged,
    *rest,
):
    rows, rhs, leaf_size, levels, rank, row_size, col_size, groups = cfg
    dev_bits = sum(bits for _, bits in groups)
    base_bits = groups[0][1]
    base = 1 << base_bits
    upper = dev_bits - base_bits
    part = rank // base
    rest = list(rest)
    low_send = [rest.pop(0) for _ in range(base_bits)]
    low_recv = [rest.pop(0) for _ in range(base_bits)]
    low_full = [rest.pop(0) for _ in range(base_bits)]
    up_send, up_recv, up_full = [rest.pop(0) for _ in range(3)]
    hold = [rest.pop(0) for _ in groups[1:]]
    recv_own = [rest.pop(0) for _ in groups[1:]]
    recv_above = [rest.pop(0) for _ in groups[1:]]
    in_sem, out_sem, send_sem, recv_sem = rest

    me = lax.axis_index("row") * col_size + lax.axis_index("col")
    mine = lax.rem(me, base)

    loads = []
    half = rows // 2
    for at, (a, b) in enumerate(
        [(v_hbm, v)]
        + [(src_hbm.at[pl.ds(h * half, half)], src.at[pl.ds(h * half, half)]) for h in range(2)]
        + [(u_hbm, u), (leaf_hbm, leaf)]
    ):
        copy = pltpu.make_async_copy(a, b, in_sem.at[at])
        copy.start()
        loads.append(copy)

    barrier = pltpu.get_barrier_semaphore()
    partners = [k << start for start, bits in groups for k in range(1, 1 << bits)]

    def device(mask):
        other = flip(me, mask)
        return (lax.div(other, col_size), lax.rem(other, col_size))

    for mask in partners:
        pl.semaphore_signal(
            barrier, inc=1, device_id=device(mask), device_id_type=pl.DeviceIdType.MESH
        )

    count = [0]
    copies = []

    def send(source, target, mask):
        at = count[0]
        count[0] += 1
        copy = pltpu.make_async_remote_copy(
            src_ref=source,
            dst_ref=target,
            send_sem=send_sem.at[at],
            recv_sem=recv_sem.at[at],
            device_id=device(mask),
            device_id_type=pl.DeviceIdType.MESH,
        )
        copy.start()
        copies.append(copy)
        return copy

    local = (perm_ref[...] - me * rows).astype(F32)
    wide = jnp.broadcast_to(local, (128, rows)).T
    lane = lax.broadcasted_iota(jnp.int32, (rows, 128), 1).astype(F32)
    for c in range(rows // 128):
        one_hot[:, c * 128:(c + 1) * 128] = jnp.where(wide == lane + c * 128.0, 1.0, 0.0).astype(BF16)

    loads[0].wait()
    v_all = v[...].reshape(levels * rank, rows)
    v_perm = jnp.dot(v_all[: dev_bits * rank], one_hot[...], preferred_element_type=F32).astype(BF16)
    loads[1].wait()
    loads[2].wait()
    coef = jnp.dot(v_perm, src[...], preferred_element_type=F32)
    staged[...] = coef
    for p in range(base_bits, dev_bits):
        first = (dev_bits - 1 - p) * rank
        for q in range(base):
            up_send[q, p - base_bits] = staged[first + q * part:first + (q + 1) * part]

    pl.semaphore_wait(barrier, len(partners))
    up_copies, low_copies = {}, {}
    if upper:
        for k in reversed(range(1, base)):
            up_copies[k] = send(up_send.at[flip(mine, k)], up_recv.at[k], k)
    for p in range(base_bits):
        first = (dev_bits - 1 - p) * rank
        size = rank >> p
        for q in range(1 << p):
            low_send[p][q] = staged[first + q * size:first + (q + 1) * size]
    for k in reversed(range(1, base)):
        p = top_bit(k)
        piece = lax.rem(flip(mine, k), 1 << p)
        target = low_full[0].at[0] if p == 0 else low_recv[p].at[k - (1 << p)]
        low_copies[k] = send(low_send[p].at[piece], target, k)

    for c in range(rows // 128):
        row = lax.broadcasted_iota(jnp.int32, (128, rows), 0).astype(F32) + c * 128.0
        one_hot_t[c * 128:(c + 1) * 128, :] = jnp.where(local == row, 1.0, 0.0).astype(BF16)
    chunk = rows // 4
    for c in range(4):
        at = pl.ds(c * chunk, chunk)
        ordered[at, :] = jnp.dot(one_hot[at, :], src[...], preferred_element_type=F32).astype(BF16)

    held = None
    if upper:
        for k in reversed(range(1, base)):
            up_copies[k].wait_recv()
        total = up_send[mine]
        for k in range(1, base):
            total = total + up_recv[k]
        held = total
    own_copies, above_copies = {}, {}

    def send_group(g):
        start, bits = groups[g]
        lowest = start - base_bits
        hold[g - 1][...] = held[lowest:]
        for k in reversed(range(1, 1 << bits)):
            own_copies[g, k] = send(hold[g - 1].at[top_bit(k)], recv_own[g - 1].at[k], k << start)
            if start + bits < dev_bits:
                above_copies[g, k] = send(
                    hold[g - 1].at[pl.ds(bits, dev_bits - start - bits)], recv_above[g - 1].at[k], k << start
                )

    if len(groups) > 1:
        send_group(1)

    for k in range(1, base):
        low_copies[k].wait_recv()
    low_gather = []
    for p in range(1, base_bits):
        total = low_recv[p][0]
        for k in range(1, 1 << p):
            total = total + low_recv[p][k]
        slot = lax.rem(mine, 1 << p)
        low_full[p][slot] = total
        for k in range(1, 1 << p):
            low_gather.append(send(low_full[p].at[slot], low_full[p].at[slot], k))

    lane_all = lax.broadcasted_iota(jnp.int32, (1, dev_bits * rank), 1)
    keep = jnp.zeros((1, dev_bits * rank), F32)
    for l in range(dev_bits):
        inside = (lane_all >= l * rank) & (lane_all < l * rank + ranks_ref[l])
        keep = jnp.where(inside, 1.0, keep)
    loads[3].wait()
    u_all = u[...].reshape(levels * rank, rows)
    nt = (((1,), (1,)), ((), ()))
    for c in range(4):
        at = pl.ds(c * chunk, chunk)
        u_perm[at, :] = (
            lax.dot_general(one_hot_t[at, :], u_all[: dev_bits * rank], nt, preferred_element_type=F32) * keep
        ).astype(BF16)
    loads[4].wait()
    for c in range(4):
        at = pl.ds(c * chunk, chunk)
        for g in range(rows // leaf_size):
            cols = slice(g * leaf_size, (g + 1) * leaf_size)
            mixed[at, cols] = jnp.dot(
                one_hot_t[at, cols], leaf[cols, :], preferred_element_type=F32
            ).astype(BF16)

    far_up = [None] * upper
    for g in range(1, len(groups)):
        start, bits = groups[g]
        lowest = start - base_bits
        for k in range(1, 1 << bits):
            own_copies[g, k].wait_recv()
        for j in range(bits):
            total = recv_own[g - 1][1 << j]
            for k in range((1 << j) + 1, 2 << j):
                total = total + recv_own[g - 1][k]
            far_up[lowest + j] = total
        if start + bits < dev_bits:
            for k in range(1, 1 << bits):
                above_copies[g, k].wait_recv()
            total = held[lowest + bits:]
            for k in range(1, 1 << bits):
                total = total + recv_above[g - 1][k]
            held = jnp.concatenate([held[: lowest + bits], total], axis=0)
            send_group(g + 1)
    up_gather = []
    if upper:
        for i in range(upper):
            up_full[mine, i] = far_up[i]
        for k in reversed(range(1, base)):
            up_gather.append(send(up_full.at[mine], up_full.at[mine], k))

    near_at = 0
    for l in range(dev_bits, levels):
        cluster = rows >> l - dev_bits + 1
        for g in range(rows // cluster):
            for_u = slice(g * cluster, (g + 1) * cluster)
            sib = g ^ 1
            for_v = slice(sib * cluster, (sib + 1) * cluster)
            near[near_at:near_at + rank, :] = jnp.dot(
                v_all[l * rank:(l + 1) * rank, for_v], ordered[for_v, :], preferred_element_type=F32
            ).astype(BF16)
            inside = lax.broadcasted_iota(jnp.int32, (1, rank), 1) < ranks_ref[l]
            u_near[:, near_at:near_at + rank] = (
                lax.dot_general(
                    one_hot_t[:, for_u], u_all[l * rank:(l + 1) * rank, for_u], nt, preferred_element_type=F32
                )
                * jnp.where(inside, 1.0, 0.0)
            ).astype(BF16)
            near_at += rank
    for c in range(4):
        at = pl.ds(c * chunk, chunk)
        total = jnp.dot(mixed[at, :], ordered[...], preferred_element_type=F32)
        if near_at:
            total = total + jnp.dot(u_near[at, :], near[...], preferred_element_type=F32)
        acc[at, :] = total

    for copy in low_gather:
        copy.wait_recv()
    for p in range(base_bits):
        first = (dev_bits - 1 - p) * rank
        size = rank >> p
        for q in range(1 << p):
            far[first + q * size:first + (q + 1) * size, :] = low_full[p][q]
    for copy in up_gather:
        copy.wait_recv()
    for i in range(upper):
        first = (dev_bits - 1 - (base_bits + i)) * rank
        for q in range(base):
            far[first + q * part:first + (q + 1) * part, :] = up_full[q, i]
    far_low = far[...].astype(BF16)
    stores = []
    for c in range(4):
        at = pl.ds(c * chunk, chunk)
        total = acc[at, :] + jnp.dot(u_perm[at, :], far_low, preferred_element_type=F32)
        src[at, :] = total.astype(BF16)
        copy = pltpu.make_async_copy(src.at[at], out_hbm.at[at], out_sem.at[c])
        copy.start()
        stores.append(copy)
    for copy in copies:
        copy.wait_send()
    for copy in stores:
        copy.wait()


def per_device(sources, tree_perm, leaf_blocks, u_factors, v_factors, level_ranks):
    rows, rhs = sources.shape
    leaf_size = leaf_blocks.shape[1]
    levels, rank, _ = u_factors.shape
    row_size, col_size = lax.axis_size("row"), lax.axis_size("col")
    dev_bits = (row_size * col_size).bit_length() - 1
    groups = split_bits(dev_bits)
    base_bits = groups[0][1]
    base = 1 << base_bits
    upper = dev_bits - base_bits
    part = rank // base
    cfg = (rows, rhs, leaf_size, levels, rank, row_size, col_size, groups)
    near_rows = rank * sum(2 << i for i in range(levels - dev_bits))
    vmem = pltpu.VMEM

    low = [vmem((1 << p, rank >> p, rhs), F32) for p in range(base_bits)]
    up = max(upper, 1)
    scratch = [
        vmem((rows, rhs), BF16),
        vmem(leaf_blocks.shape, BF16),
        vmem(u_factors.shape, BF16),
        vmem(v_factors.shape, BF16),
        vmem((rows, rows), BF16),
        vmem((rows, rows), BF16),
        vmem((rows, rhs), BF16),
        vmem((rows, rows), BF16),
        vmem((rows, dev_bits * rank), BF16),
        vmem((rows, max(near_rows, rank)), BF16),
        vmem((max(near_rows, rank), rhs), BF16),
        vmem((rows, rhs), F32),
        vmem((dev_bits * rank, rhs), F32),
        vmem((dev_bits * rank, rhs), F32),
    ]
    scratch += low + low + low
    scratch += [vmem((base, up, part, rhs), F32)] * 3
    scratch += [vmem((dev_bits - start, part, rhs), F32) for start, _ in groups[1:]]
    scratch += [vmem((1 << bits, part, rhs), F32) for _, bits in groups[1:]]
    scratch += [
        vmem((1 << bits, max(dev_bits - start - bits, 1), part, rhs), F32) for start, bits in groups[1:]
    ]
    total = (3 if upper else 1) * base + base + 2 * sum(1 << bits for _, bits in groups[1:])
    scratch += [
        pltpu.SemaphoreType.DMA((5,)),
        pltpu.SemaphoreType.DMA((4,)),
        pltpu.SemaphoreType.DMA((total,)),
        pltpu.SemaphoreType.DMA((total,)),
    ]
    any_space = pl.BlockSpec(memory_space=pl.ANY)
    return pl.pallas_call(
        functools.partial(kernel, cfg),
        out_shape=jax.ShapeDtypeStruct((rows, rhs), BF16),
        in_specs=[
            pl.BlockSpec(memory_space=pltpu.SMEM),
            pl.BlockSpec(memory_space=pltpu.VMEM),
            any_space, any_space, any_space, any_space,
        ],
        out_specs=any_space,
        scratch_shapes=scratch,
        compiler_params=pltpu.CompilerParams(
            collective_id=0, has_side_effects=True, vmem_limit_bytes=56 * 1024 * 1024
        ),
    )(level_ranks, tree_perm.reshape(1, rows), sources, leaf_blocks, u_factors, v_factors)


def solution(mesh):
    placed = (
        P(("row", "col"), None),
        P(("row", "col")),
        P(("row", "col"), None),
        P(None, None, ("row", "col")),
        P(None, None, ("row", "col")),
        P(),
    )
    return jax.shard_map(
        per_device, mesh=mesh, in_specs=placed, out_specs=P(("row", "col"), None), check_vma=False
    )
```

```python
import functools

import jax
import jax.numpy as jnp
from jax import lax
from jax.experimental import pallas as pl
from jax.experimental.pallas import tpu as pltpu
from jax.sharding import PartitionSpec as P

F32 = jnp.float32
BF16 = jnp.bfloat16
VMEM_BYTES = 67043328


def flip(x, mask):
    bit = 0
    while mask >> bit:
        if mask >> bit & 1:
            x = x + (1 << bit) * (1 - 2 * lax.rem(lax.div(x, 1 << bit), 2))
        bit += 1
    return x


def split_bits(dev_bits):
    groups, start = [], 0
    while start < dev_bits:
        bits = min(3, dev_bits - start)
        groups.append((start, bits))
        start += bits
    return groups


def top_bit(k):
    return k.bit_length() - 1


def kernel(
    cfg,
    ranks_ref, perm_ref, src_hbm, leaf_hbm, u_hbm, v_hbm,
    acc, u_perm, far,
    src, leaf, u, v, one_hot, one_hot_t, ordered, mixed, u_near, near, staged,
    *rest,
):
    rows, rhs, leaf_size, levels, rank, row_size, col_size, groups = cfg
    dev_bits = sum(bits for _, bits in groups)
    base_bits = groups[0][1]
    base = 1 << base_bits
    upper = dev_bits - base_bits
    part = rank // base
    rest = list(rest)
    low_send = [rest.pop(0) for _ in range(base_bits)]
    low_recv = [rest.pop(0) for _ in range(base_bits)]
    low_full = [rest.pop(0) for _ in range(base_bits)]
    up_send, up_recv, up_full = [rest.pop(0) for _ in range(3)]
    hold = [rest.pop(0) for _ in groups[1:]]
    recv_own = [rest.pop(0) for _ in groups[1:]]
    recv_above = [rest.pop(0) for _ in groups[1:]]
    in_sem, send_sem, recv_sem = rest

    me = lax.axis_index("row") * col_size + lax.axis_index("col")
    mine = lax.rem(me, base)

    loads = []
    half = rows // 2
    for at, (a, b) in enumerate(
        [(v_hbm, v)]
        + [(src_hbm.at[pl.ds(h * half, half)], src.at[pl.ds(h * half, half)]) for h in range(2)]
        + [(u_hbm, u), (leaf_hbm, leaf)]
    ):
        copy = pltpu.make_async_copy(a, b, in_sem.at[at])
        copy.start()
        loads.append(copy)

    barrier = pltpu.get_barrier_semaphore()
    partners = [k << start for start, bits in groups for k in range(1, 1 << bits)]

    def device(mask):
        other = flip(me, mask)
        return (lax.div(other, col_size), lax.rem(other, col_size))

    for mask in partners:
        pl.semaphore_signal(
            barrier, inc=1, device_id=device(mask), device_id_type=pl.DeviceIdType.MESH
        )

    count = [0]
    copies = []

    def send(source, target, mask):
        at = count[0]
        count[0] += 1
        copy = pltpu.make_async_remote_copy(
            src_ref=source,
            dst_ref=target,
            send_sem=send_sem.at[at],
            recv_sem=recv_sem.at[at],
            device_id=device(mask),
            device_id_type=pl.DeviceIdType.MESH,
        )
        copy.start()
        copies.append(copy)
        return copy

    local = (perm_ref[...] - me * rows).astype(F32)
    wide = jnp.broadcast_to(local, (128, rows)).T
    lane = lax.broadcasted_iota(jnp.int32, (rows, 128), 1).astype(F32)
    for c in range(rows // 128):
        one_hot[:, c * 128:(c + 1) * 128] = jnp.where(wide == lane + c * 128.0, 1.0, 0.0).astype(BF16)

    loads[0].wait()
    v_all = v[...].reshape(levels * rank, rows)
    v_perm = jnp.dot(v_all[: dev_bits * rank], one_hot[...], preferred_element_type=F32).astype(BF16)
    loads[1].wait()
    loads[2].wait()
    coef = jnp.dot(v_perm, src[...], preferred_element_type=F32)
    staged[...] = coef
    for p in range(base_bits, dev_bits):
        first = (dev_bits - 1 - p) * rank
        for q in range(base):
            up_send[p - base_bits, q] = staged[first + q * part:first + (q + 1) * part]

    pl.semaphore_wait(barrier, len(partners))
    up_copies, low_copies = {}, {}
    if upper:
        for i in reversed(range(upper)):
            for k in reversed(range(1, base)):
                up_copies[i, k] = send(up_send.at[i, flip(mine, k)], up_recv.at[i, k], k)
    for p in range(base_bits):
        first = (dev_bits - 1 - p) * rank
        size = rank >> p
        for q in range(1 << p):
            low_send[p][q] = staged[first + q * size:first + (q + 1) * size]
    for k in reversed(range(1, base)):
        p = top_bit(k)
        piece = lax.rem(flip(mine, k), 1 << p)
        target = low_full[0].at[0] if p == 0 else low_recv[p].at[k - (1 << p)]
        low_copies[k] = send(low_send[p].at[piece], target, k)

    for c in range(rows // 128):
        row = lax.broadcasted_iota(jnp.int32, (128, rows), 0).astype(F32) + c * 128.0
        one_hot_t[c * 128:(c + 1) * 128, :] = jnp.where(local == row, 1.0, 0.0).astype(BF16)
    chunk = rows // 4
    for c in range(4):
        at = pl.ds(c * chunk, chunk)
        ordered[at, :] = jnp.dot(one_hot[at, :], src[...], preferred_element_type=F32).astype(BF16)

    own_copies, above_copies, up_gather = {}, {}, {}

    def plane_sum(i):
        for k in reversed(range(1, base)):
            up_copies[i, k].wait_recv()
        total = up_send[i, mine]
        for k in range(1, base):
            total = total + up_recv[i, k]
        return total

    def send_group(g, i, value):
        start, bits = groups[g]
        at = i - (start - base_bits)
        hold[g - 1][at] = value
        if at < bits:
            for k in reversed(range(1 << at, 2 << at)):
                own_copies[g, k] = send(hold[g - 1].at[at], recv_own[g - 1].at[k], k << start)
        else:
            for k in reversed(range(1, 1 << bits)):
                above_copies[g, i, k] = send(
                    hold[g - 1].at[at], recv_above[g - 1].at[at - bits, k], k << start
                )

    def gather_level(g, j):
        i = groups[g][0] - base_bits + j
        total = None
        for k in range(1 << j, 2 << j):
            own_copies[g, k].wait_recv()
            total = recv_own[g - 1][k] if total is None else total + recv_own[g - 1][k]
        up_full[i, mine] = total
        for k in reversed(range(1, base)):
            up_gather[i, k] = send(up_full.at[i, mine], up_full.at[i, mine], k)

    for i in reversed(range(upper)):
        send_group(1, i, plane_sum(i))

    lane_all = lax.broadcasted_iota(jnp.int32, (1, dev_bits * rank), 1)
    keep = jnp.zeros((1, dev_bits * rank), F32)
    for l in range(dev_bits):
        inside = (lane_all >= l * rank) & (lane_all < l * rank + ranks_ref[l])
        keep = jnp.where(inside, 1.0, keep)
    loads[3].wait()
    u_all = u[...].reshape(levels * rank, rows)
    nt = (((1,), (1,)), ((), ()))
    for c in range(4):
        at = pl.ds(c * chunk, chunk)
        u_perm[at, :] = (
            lax.dot_general(one_hot_t[at, :], u_all[: dev_bits * rank], nt, preferred_element_type=F32) * keep
        ).astype(BF16)
    loads[4].wait()

    def mix():
        for c in range(4):
            at = pl.ds(c * chunk, chunk)
            for g in range(rows // leaf_size):
                cols = slice(g * leaf_size, (g + 1) * leaf_size)
                mixed[at, cols] = jnp.dot(
                    one_hot_t[at, cols], leaf[cols, :], preferred_element_type=F32
                ).astype(BF16)

    low_gather = []

    def low_levels():
        for k in range(1, base):
            low_copies[k].wait_recv()
        for p in range(1, base_bits):
            total = low_recv[p][0]
            for k in range(1, 1 << p):
                total = total + low_recv[p][k]
            slot = lax.rem(mine, 1 << p)
            low_full[p][slot] = total
            for k in range(1, 1 << p):
                low_gather.append(send(low_full[p].at[slot], low_full[p].at[slot], k))

    def near_levels():
        near_at = 0
        for l in range(dev_bits, levels):
            cluster = rows >> l - dev_bits + 1
            for g in range(rows // cluster):
                for_u = slice(g * cluster, (g + 1) * cluster)
                sib = g ^ 1
                for_v = slice(sib * cluster, (sib + 1) * cluster)
                near[near_at:near_at + rank, :] = jnp.dot(
                    v_all[l * rank:(l + 1) * rank, for_v], ordered[for_v, :], preferred_element_type=F32
                ).astype(BF16)
                inside = lax.broadcasted_iota(jnp.int32, (1, rank), 1) < ranks_ref[l]
                u_near[:, near_at:near_at + rank] = (
                    lax.dot_general(
                        one_hot_t[:, for_u], u_all[l * rank:(l + 1) * rank, for_u], nt, preferred_element_type=F32
                    )
                    * jnp.where(inside, 1.0, 0.0)
                ).astype(BF16)
                near_at += rank

    def apply_rows(c):
        at = pl.ds(c * chunk, chunk)
        total = jnp.dot(mixed[at, :], ordered[...], preferred_element_type=F32)
        if levels > dev_bits:
            total = total + jnp.dot(u_near[at, :], near[...], preferred_element_type=F32)
        acc[at, :] = total

    fillers = [mix, low_levels, near_levels] + [functools.partial(apply_rows, c) for c in range(4)]
    fillers.pop(0)()
    for g in range(1, len(groups)):
        start, bits = groups[g]
        for i in reversed(range(start + bits - base_bits, upper)):
            total = hold[g - 1][i - (start - base_bits)]
            for k in reversed(range(1, 1 << bits)):
                above_copies[g, i, k].wait_recv()
                total = total + recv_above[g - 1][i - (start + bits - base_bits), k]
            send_group(g + 1, i, total)
        for j in range(bits):
            gather_level(g, j)
            for _ in range(2):
                if fillers and j < bits - 1:
                    fillers.pop(0)()
    for filler in fillers:
        filler()

    for copy in low_gather:
        copy.wait_recv()
    for p in range(base_bits):
        first = (dev_bits - 1 - p) * rank
        size = rank >> p
        for q in range(1 << p):
            staged[first + q * size:first + (q + 1) * size, :] = low_full[p][q]
    for i in range(upper):
        for k in range(1, base):
            up_gather[i, k].wait_recv()
        first = (dev_bits - 1 - (base_bits + i)) * rank
        for q in range(base):
            staged[first + q * part:first + (q + 1) * part, :] = up_full[i, q]
    far[...] = staged[...].astype(BF16)
    for copy in copies:
        copy.wait_send()


def finish(acc, u_perm, far, out_hbm, out, out_sem):
    chunk = acc.shape[0] // 4
    stores = []
    for c in range(4):
        at = pl.ds(c * chunk, chunk)
        total = acc[at, :] + jnp.dot(u_perm[at, :], far[...], preferred_element_type=F32)
        out[at, :] = total.astype(BF16)
        copy = pltpu.make_async_copy(out.at[at], out_hbm.at[at], out_sem.at[c])
        copy.start()
        stores.append(copy)
    for copy in stores:
        copy.wait()


def per_device(sources, tree_perm, leaf_blocks, u_factors, v_factors, level_ranks):
    rows, rhs = sources.shape
    leaf_size = leaf_blocks.shape[1]
    levels, rank, _ = u_factors.shape
    row_size, col_size = lax.axis_size("row"), lax.axis_size("col")
    dev_bits = (row_size * col_size).bit_length() - 1
    groups = split_bits(dev_bits)
    base_bits = groups[0][1]
    base = 1 << base_bits
    upper = dev_bits - base_bits
    part = rank // base
    cfg = (rows, rhs, leaf_size, levels, rank, row_size, col_size, groups)
    near_rows = rank * sum(2 << i for i in range(levels - dev_bits))
    vmem = pltpu.VMEM

    low = [vmem((1 << p, rank >> p, rhs), F32) for p in range(base_bits)]
    up = max(upper, 1)
    scratch = [
        vmem((rows, rhs), BF16),
        vmem(leaf_blocks.shape, BF16),
        vmem(u_factors.shape, BF16),
        vmem(v_factors.shape, BF16),
        vmem((rows, rows), BF16),
        vmem((rows, rows), BF16),
        vmem((rows, rhs), BF16),
        vmem((rows, rows), BF16),
        vmem((rows, max(near_rows, rank)), BF16),
        vmem((max(near_rows, rank), rhs), BF16),
        vmem((dev_bits * rank, rhs), F32),
    ]
    scratch += low + low + low
    scratch += [vmem((up, base, part, rhs), F32)] * 3
    scratch += [vmem((dev_bits - start, part, rhs), F32) for start, _ in groups[1:]]
    scratch += [vmem((1 << bits, part, rhs), F32) for _, bits in groups[1:]]
    scratch += [
        vmem((max(dev_bits - start - bits, 1), 1 << bits, part, rhs), F32) for start, bits in groups[1:]
    ]
    total = (2 * upper + 2) * base + sum((dev_bits - start) << bits for start, bits in groups[1:])
    scratch += [
        pltpu.SemaphoreType.DMA((5,)),
        pltpu.SemaphoreType.DMA((total,)),
        pltpu.SemaphoreType.DMA((total,)),
    ]
    wide = -(-dev_bits * rank // 128) * 128
    kept = rows * rhs * 4 + rows * wide * 2 + dev_bits * rank * rhs * 2
    any_space = pl.BlockSpec(memory_space=pl.ANY)
    vmem_space = pl.BlockSpec(memory_space=pltpu.VMEM)
    acc, u_perm, far = pl.pallas_call(
        functools.partial(kernel, cfg),
        out_shape=(
            pltpu.VMEM((rows, rhs), F32),
            pltpu.VMEM((rows, dev_bits * rank), BF16),
            pltpu.VMEM((dev_bits * rank, rhs), BF16),
        ),
        in_specs=[
            pl.BlockSpec(memory_space=pltpu.SMEM), vmem_space,
            any_space, any_space, any_space, any_space,
        ],
        out_specs=(vmem_space, vmem_space, vmem_space),
        scratch_shapes=scratch,
        compiler_params=pltpu.CompilerParams(
            collective_id=0, has_side_effects=True, vmem_limit_bytes=VMEM_BYTES - kept - 96 * 1024
        ),
    )(level_ranks, tree_perm.reshape(1, rows), sources, leaf_blocks, u_factors, v_factors)
    return pl.pallas_call(
        finish,
        out_shape=jax.ShapeDtypeStruct((rows, rhs), BF16),
        in_specs=[vmem_space, vmem_space, vmem_space],
        out_specs=any_space,
        scratch_shapes=[vmem((rows, rhs), BF16), pltpu.SemaphoreType.DMA((4,))],
        compiler_params=pltpu.CompilerParams(vmem_limit_bytes=8 * 1024 * 1024),
    )(acc, u_perm, far)


def solution(mesh):
    placed = (
        P(("row", "col"), None),
        P(("row", "col")),
        P(("row", "col"), None),
        P(None, None, ("row", "col")),
        P(None, None, ("row", "col")),
        P(),
    )
    return jax.shard_map(
        per_device, mesh=mesh, in_specs=placed, out_specs=P(("row", "col"), None), check_vma=False
    )
```

```python
import functools

import jax
import jax.numpy as jnp
from jax import lax
from jax.experimental import pallas as pl
from jax.experimental.pallas import tpu as pltpu
from jax.sharding import PartitionSpec as P

F32 = jnp.float32
BF16 = jnp.bfloat16
VMEM_BYTES = 67043328


def flip(x, mask):
    bit = 0
    while mask >> bit:
        if mask >> bit & 1:
            x = x + (1 << bit) * (1 - 2 * lax.rem(lax.div(x, 1 << bit), 2))
        bit += 1
    return x


def split_bits(dev_bits):
    groups, start = [], 0
    while start < dev_bits:
        bits = min(3, dev_bits - start)
        groups.append((start, bits))
        start += bits
    return groups


def top_bit(k):
    return k.bit_length() - 1


def kernel(
    cfg,
    ranks_hbm, perm_hbm, src_hbm, leaf_hbm, u_hbm, v_hbm,
    acc, u_perm, far,
    src, leaf, u, v, one_hot, one_hot_t, ordered, mixed, u_near, near, staged,
    *rest,
):
    rows, rhs, leaf_size, levels, rank, row_size, col_size, groups = cfg
    dev_bits = sum(bits for _, bits in groups)
    base_bits = groups[0][1]
    base = 1 << base_bits
    upper = dev_bits - base_bits
    part = rank // base
    rest = list(rest)
    low_send = [rest.pop(0) for _ in range(base_bits)]
    low_recv = [rest.pop(0) for _ in range(base_bits)]
    low_full = [rest.pop(0) for _ in range(base_bits)]
    low_chip = [rest.pop(0) for _ in range(base_bits)]
    low_sum = [rest.pop(0) for _ in range(base_bits)]
    up_send, up_recv, up_full = [rest.pop(0) for _ in range(3)]
    hold = [rest.pop(0) for _ in groups[1:]]
    recv_own = [rest.pop(0) for _ in groups[1:]]
    recv_above = [rest.pop(0) for _ in groups[1:]]
    ranks_ref, perm_ref, in_sem, send_sem, recv_sem = rest

    me = lax.axis_index("row") * col_size + lax.axis_index("col")
    mine = lax.rem(me, base)

    half = rows // 2
    loads = [
        pltpu.make_async_copy(a, b, in_sem.at[at])
        for at, (a, b) in enumerate(
            [(perm_hbm, perm_ref), (v_hbm, v)]
            + [(src_hbm.at[pl.ds(h * half, half)], src.at[pl.ds(h * half, half)]) for h in range(2)]
            + [(ranks_hbm, ranks_ref), (u_hbm, u), (leaf_hbm, leaf)]
        )
    ]
    for copy in loads[:4]:
        copy.start()

    barrier = pltpu.get_barrier_semaphore()
    partners = [k << start for start, bits in groups for k in range(1, 1 << bits)]

    def device(mask):
        other = flip(me, mask)
        return (lax.div(other, col_size), lax.rem(other, col_size))

    for mask in partners:
        pl.semaphore_signal(
            barrier, inc=1, device_id=device(mask), device_id_type=pl.DeviceIdType.MESH
        )

    count = [0]
    copies = []

    def send(source, target, mask):
        at = count[0]
        count[0] += 1
        copy = pltpu.make_async_remote_copy(
            src_ref=source,
            dst_ref=target,
            send_sem=send_sem.at[at],
            recv_sem=recv_sem.at[at],
            device_id=device(mask),
            device_id_type=pl.DeviceIdType.MESH,
        )
        copy.start()
        copies.append(copy)
        return copy

    loads[0].wait()
    local = (perm_ref[...] - me * rows).astype(F32)
    wide = jnp.broadcast_to(local, (128, rows)).T
    lane = lax.broadcasted_iota(jnp.int32, (rows, 128), 1).astype(F32)
    for c in range(rows // 128):
        one_hot[:, c * 128:(c + 1) * 128] = jnp.where(wide == lane + c * 128.0, 1.0, 0.0).astype(BF16)

    loads[1].wait()
    v_all = v[...].reshape(levels * rank, rows)
    v_perm = jnp.dot(v_all[: dev_bits * rank], one_hot[...], preferred_element_type=F32).astype(BF16)
    loads[2].wait()
    loads[3].wait()
    for copy in loads[4:]:
        copy.start()
    coef = jnp.dot(v_perm, src[...], preferred_element_type=F32)
    staged[...] = coef
    for p in range(base_bits, dev_bits):
        first = (dev_bits - 1 - p) * rank
        for q in range(base):
            up_send[p - base_bits, q] = staged[first + q * part:first + (q + 1) * part]

    pl.semaphore_wait(barrier, len(partners))
    up_copies, low_copies = {}, {}
    if upper:
        for i in reversed(range(upper)):
            for k in reversed(range(1, base)):
                up_copies[i, k] = send(up_send.at[i, flip(mine, k)], up_recv.at[i, k], k)
    chip_copies = {}
    bit = lax.rem(me, 2)
    for p in range(base_bits):
        first = (dev_bits - 1 - p) * rank
        size = rank >> p
        if p == 0:
            low_send[0][0] = staged[first:first + size]
            low_copies[1] = send(low_send[0].at[0], low_full[0].at[0], 1)
            continue
        for q in range(1 << p):
            low_send[p][q % 2, q // 2] = staged[first + q * size:first + (q + 1) * size]
        chip_copies[p] = send(low_send[p].at[1 - bit], low_chip[p], 1)

    for c in range(rows // 128):
        row = lax.broadcasted_iota(jnp.int32, (128, rows), 0).astype(F32) + c * 128.0
        one_hot_t[c * 128:(c + 1) * 128, :] = jnp.where(local == row, 1.0, 0.0).astype(BF16)
    chunk = rows // 4

    def order_rows(c):
        at = pl.ds(c * chunk, chunk)
        ordered[at, :] = jnp.dot(one_hot[at, :], src[...], preferred_element_type=F32).astype(BF16)

    order_rows(0)
    order_rows(1)

    for p in range(1, base_bits):
        chip_copies[p].wait_recv()
        low_sum[p][...] = low_send[p][bit] + low_chip[p][...]
        for k in reversed(range(1 << p, 2 << p, 2)):
            piece = lax.div(lax.rem(flip(mine, k), 1 << p), 2)
            low_copies[k] = send(low_sum[p].at[piece], low_recv[p].at[(k - (1 << p)) // 2], k)
    order_rows(2)
    order_rows(3)

    own_copies, above_copies, up_gather = {}, {}, {}

    def plane_sum(i):
        for k in reversed(range(1, base)):
            up_copies[i, k].wait_recv()
        total = up_send[i, mine]
        for k in range(1, base):
            total = total + up_recv[i, k]
        return total

    def send_group(g, i, value):
        start, bits = groups[g]
        at = i - (start - base_bits)
        hold[g - 1][at] = value
        if at < bits:
            for k in reversed(range(1 << at, 2 << at)):
                own_copies[g, k] = send(hold[g - 1].at[at], recv_own[g - 1].at[k], k << start)
        else:
            for k in reversed(range(1, 1 << bits)):
                above_copies[g, i, k] = send(
                    hold[g - 1].at[at], recv_above[g - 1].at[at - bits, k], k << start
                )

    def gather_level(g, j):
        i = groups[g][0] - base_bits + j
        total = None
        for k in range(1 << j, 2 << j):
            own_copies[g, k].wait_recv()
            total = recv_own[g - 1][k] if total is None else total + recv_own[g - 1][k]
        up_full[i, mine] = total
        for k in reversed(range(1, base)):
            up_gather[i, k] = send(up_full.at[i, mine], up_full.at[i, mine], k)

    for i in reversed(range(upper)):
        send_group(1, i, plane_sum(i))

    loads[4].wait()
    lane_all = lax.broadcasted_iota(jnp.int32, (1, dev_bits * rank), 1)
    keep = jnp.zeros((1, dev_bits * rank), F32)
    for l in range(dev_bits):
        inside = (lane_all >= l * rank) & (lane_all < l * rank + ranks_ref[l])
        keep = jnp.where(inside, 1.0, keep)
    loads[5].wait()
    u_all = u[...].reshape(levels * rank, rows)
    nt = (((1,), (1,)), ((), ()))
    for c in range(4):
        at = pl.ds(c * chunk, chunk)
        u_perm[at, :] = (
            lax.dot_general(one_hot_t[at, :], u_all[: dev_bits * rank], nt, preferred_element_type=F32) * keep
        ).astype(BF16)
    loads[6].wait()

    def mix():
        for c in range(4):
            at = pl.ds(c * chunk, chunk)
            for g in range(rows // leaf_size):
                cols = slice(g * leaf_size, (g + 1) * leaf_size)
                mixed[at, cols] = jnp.dot(
                    one_hot_t[at, cols], leaf[cols, :], preferred_element_type=F32
                ).astype(BF16)

    low_gather = []

    def low_levels():
        for copy in low_copies.values():
            copy.wait_recv()
        for p in range(1, base_bits):
            total = low_recv[p][0]
            for k in range(1, 1 << p - 1):
                total = total + low_recv[p][k]
            slot = lax.rem(mine, 1 << p)
            low_full[p][slot] = total
            for k in range(1, 1 << p):
                low_gather.append(send(low_full[p].at[slot], low_full[p].at[slot], k))

    def near_levels():
        near_at = 0
        for l in range(dev_bits, levels):
            cluster = rows >> l - dev_bits + 1
            for g in range(rows // cluster):
                for_u = slice(g * cluster, (g + 1) * cluster)
                sib = g ^ 1
                for_v = slice(sib * cluster, (sib + 1) * cluster)
                near[near_at:near_at + rank, :] = jnp.dot(
                    v_all[l * rank:(l + 1) * rank, for_v], ordered[for_v, :], preferred_element_type=F32
                ).astype(BF16)
                inside = lax.broadcasted_iota(jnp.int32, (1, rank), 1) < ranks_ref[l]
                u_near[:, near_at:near_at + rank] = (
                    lax.dot_general(
                        one_hot_t[:, for_u], u_all[l * rank:(l + 1) * rank, for_u], nt, preferred_element_type=F32
                    )
                    * jnp.where(inside, 1.0, 0.0)
                ).astype(BF16)
                near_at += rank

    def apply_rows(c):
        at = pl.ds(c * chunk, chunk)
        total = jnp.dot(mixed[at, :], ordered[...], preferred_element_type=F32)
        if levels > dev_bits:
            total = total + jnp.dot(u_near[at, :], near[...], preferred_element_type=F32)
        acc[at, :] = total

    fillers = [mix, low_levels, near_levels] + [functools.partial(apply_rows, c) for c in range(4)]
    fillers.pop(0)()
    for g in range(1, len(groups)):
        start, bits = groups[g]
        for i in reversed(range(start + bits - base_bits, upper)):
            total = hold[g - 1][i - (start - base_bits)]
            for k in reversed(range(1, 1 << bits)):
                above_copies[g, i, k].wait_recv()
                total = total + recv_above[g - 1][i - (start + bits - base_bits), k]
            send_group(g + 1, i, total)
        for j in range(bits):
            gather_level(g, j)
            for _ in range(2):
                if fillers and j < bits - 1:
                    fillers.pop(0)()
    for filler in fillers:
        filler()

    for copy in low_gather:
        copy.wait_recv()
    for p in range(base_bits):
        first = (dev_bits - 1 - p) * rank
        size = rank >> p
        for q in range(1 << p):
            staged[first + q * size:first + (q + 1) * size, :] = low_full[p][q]
    for i in range(upper):
        for k in range(1, base):
            up_gather[i, k].wait_recv()
        first = (dev_bits - 1 - (base_bits + i)) * rank
        for q in range(base):
            staged[first + q * part:first + (q + 1) * part, :] = up_full[i, q]
    far[...] = staged[...].astype(BF16)
    for copy in copies:
        copy.wait_send()


def finish(acc, u_perm, far, out_hbm, out, out_sem):
    chunk = acc.shape[0] // 4
    stores = []
    for c in range(4):
        at = pl.ds(c * chunk, chunk)
        total = acc[at, :] + jnp.dot(u_perm[at, :], far[...], preferred_element_type=F32)
        out[at, :] = total.astype(BF16)
        copy = pltpu.make_async_copy(out.at[at], out_hbm.at[at], out_sem.at[c])
        copy.start()
        stores.append(copy)
    for copy in stores:
        copy.wait()


def per_device(sources, tree_perm, leaf_blocks, u_factors, v_factors, level_ranks):
    rows, rhs = sources.shape
    leaf_size = leaf_blocks.shape[1]
    levels, rank, _ = u_factors.shape
    row_size, col_size = lax.axis_size("row"), lax.axis_size("col")
    dev_bits = (row_size * col_size).bit_length() - 1
    groups = split_bits(dev_bits)
    base_bits = groups[0][1]
    base = 1 << base_bits
    upper = dev_bits - base_bits
    part = rank // base
    cfg = (rows, rhs, leaf_size, levels, rank, row_size, col_size, groups)
    near_rows = rank * sum(2 << i for i in range(levels - dev_bits))
    vmem = pltpu.VMEM

    low = [vmem((1 << p, rank >> p, rhs), F32) for p in range(base_bits)]
    low_pairs = [vmem((1, rank, rhs), F32)] + [vmem((2, 1 << p - 1, rank >> p, rhs), F32) for p in range(1, base_bits)]
    low_half = [vmem((max(1 << p >> 1, 1), rank >> p, rhs), F32) for p in range(base_bits)]
    up = max(upper, 1)
    scratch = [
        vmem((rows, rhs), BF16),
        vmem(leaf_blocks.shape, BF16),
        vmem(u_factors.shape, BF16),
        vmem(v_factors.shape, BF16),
        vmem((rows, rows), BF16),
        vmem((rows, rows), BF16),
        vmem((rows, rhs), BF16),
        vmem((rows, rows), BF16),
        vmem((rows, max(near_rows, rank)), BF16),
        vmem((max(near_rows, rank), rhs), BF16),
        vmem((dev_bits * rank, rhs), F32),
    ]
    scratch += low_pairs + low_half + low + low_half + low_half
    scratch += [vmem((up, base, part, rhs), F32)] * 3
    scratch += [vmem((dev_bits - start, part, rhs), F32) for start, _ in groups[1:]]
    scratch += [vmem((1 << bits, part, rhs), F32) for _, bits in groups[1:]]
    scratch += [
        vmem((max(dev_bits - start - bits, 1), 1 << bits, part, rhs), F32) for start, bits in groups[1:]
    ]
    total = (2 * upper + 2) * base + sum((dev_bits - start) << bits for start, bits in groups[1:])
    scratch += [
        pltpu.SMEM(level_ranks.shape, jnp.int32),
        vmem((1, rows), jnp.int32),
        pltpu.SemaphoreType.DMA((7,)),
        pltpu.SemaphoreType.DMA((total,)),
        pltpu.SemaphoreType.DMA((total,)),
    ]
    wide = -(-dev_bits * rank // 128) * 128
    kept = rows * rhs * 4 + rows * wide * 2 + dev_bits * rank * rhs * 2
    any_space = pl.BlockSpec(memory_space=pl.ANY)
    vmem_space = pl.BlockSpec(memory_space=pltpu.VMEM)
    acc, u_perm, far = pl.pallas_call(
        functools.partial(kernel, cfg),
        out_shape=(
            pltpu.VMEM((rows, rhs), F32),
            pltpu.VMEM((rows, dev_bits * rank), BF16),
            pltpu.VMEM((dev_bits * rank, rhs), BF16),
        ),
        in_specs=[any_space] * 6,
        out_specs=(vmem_space, vmem_space, vmem_space),
        scratch_shapes=scratch,
        compiler_params=pltpu.CompilerParams(
            collective_id=0, has_side_effects=True, vmem_limit_bytes=VMEM_BYTES - kept - 96 * 1024
        ),
    )(level_ranks, tree_perm.reshape(1, rows), sources, leaf_blocks, u_factors, v_factors)
    return pl.pallas_call(
        finish,
        out_shape=jax.ShapeDtypeStruct((rows, rhs), BF16),
        in_specs=[vmem_space, vmem_space, vmem_space],
        out_specs=any_space,
        scratch_shapes=[vmem((rows, rhs), BF16), pltpu.SemaphoreType.DMA((4,))],
        compiler_params=pltpu.CompilerParams(vmem_limit_bytes=8 * 1024 * 1024),
    )(acc, u_perm, far)


def solution(mesh):
    placed = (
        P(("row", "col"), None),
        P(("row", "col")),
        P(("row", "col"), None),
        P(None, None, ("row", "col")),
        P(None, None, ("row", "col")),
        P(),
    )
    return jax.shard_map(
        per_device, mesh=mesh, in_specs=placed, out_specs=P(("row", "col"), None), check_vma=False
    )
```

```python
import functools

import jax
import jax.numpy as jnp
from jax import lax
from jax.experimental import pallas as pl
from jax.experimental.pallas import tpu as pltpu
from jax.sharding import PartitionSpec as P

F32 = jnp.float32
BF16 = jnp.bfloat16
VMEM_BYTES = 67043328


def flip(x, mask):
    bit = 0
    while mask >> bit:
        if mask >> bit & 1:
            x = x + (1 << bit) * (1 - 2 * lax.rem(lax.div(x, 1 << bit), 2))
        bit += 1
    return x


def split_bits(dev_bits):
    groups, start = [], 0
    while start < dev_bits:
        bits = min(3, dev_bits - start)
        groups.append((start, bits))
        start += bits
    return groups


def top_bit(k):
    return k.bit_length() - 1


def kernel(
    cfg,
    ranks_hbm, perm_hbm, src_hbm, leaf_hbm, u_hbm, v_hbm,
    acc, u_perm, far,
    src, leaf, u, v, one_hot, one_hot_t, ordered, mixed, u_near, near, staged,
    *rest,
):
    rows, rhs, leaf_size, levels, rank, row_size, col_size, groups = cfg
    dev_bits = sum(bits for _, bits in groups)
    base_bits = groups[0][1]
    base = 1 << base_bits
    upper = dev_bits - base_bits
    part = rank // base
    rest = list(rest)
    low_send = [rest.pop(0) for _ in range(base_bits)]
    low_recv = [rest.pop(0) for _ in range(base_bits)]
    low_full = [rest.pop(0) for _ in range(base_bits)]
    low_chip = [rest.pop(0) for _ in range(base_bits)]
    low_sum = [rest.pop(0) for _ in range(base_bits)]
    up_send, up_recv, up_full = [rest.pop(0) for _ in range(3)]
    hold = [rest.pop(0) for _ in groups[1:]]
    recv_own = [rest.pop(0) for _ in groups[1:]]
    recv_above = [rest.pop(0) for _ in groups[1:]]
    ranks_ref, perm_ref, in_sem, send_sem, recv_sem = rest

    me = lax.axis_index("row") * col_size + lax.axis_index("col")
    mine = lax.rem(me, base)

    half = rows // 2
    loads = [
        pltpu.make_async_copy(a, b, in_sem.at[at])
        for at, (a, b) in enumerate(
            [(perm_hbm, perm_ref), (v_hbm, v)]
            + [(src_hbm.at[pl.ds(h * half, half)], src.at[pl.ds(h * half, half)]) for h in range(2)]
            + [(ranks_hbm, ranks_ref), (u_hbm, u), (leaf_hbm, leaf)]
        )
    ]
    for copy in loads[:4]:
        copy.start()

    barrier = pltpu.get_barrier_semaphore()
    partners = [k << start for start, bits in groups for k in range(1, 1 << bits)]

    def device(mask):
        other = flip(me, mask)
        return (lax.div(other, col_size), lax.rem(other, col_size))

    for mask in partners:
        pl.semaphore_signal(
            barrier, inc=1, device_id=device(mask), device_id_type=pl.DeviceIdType.MESH
        )

    count = [0]
    copies = []

    def send(source, target, mask):
        at = count[0]
        count[0] += 1
        copy = pltpu.make_async_remote_copy(
            src_ref=source,
            dst_ref=target,
            send_sem=send_sem.at[at],
            recv_sem=recv_sem.at[at],
            device_id=device(mask),
            device_id_type=pl.DeviceIdType.MESH,
        )
        copy.start()
        copies.append(copy)
        return copy

    loads[0].wait()
    local = (perm_ref[...] - me * rows).astype(F32)
    wide = jnp.broadcast_to(local, (128, rows)).T
    lane = lax.broadcasted_iota(jnp.int32, (rows, 128), 1).astype(F32)
    for c in range(rows // 128):
        one_hot[:, c * 128:(c + 1) * 128] = jnp.where(wide == lane + c * 128.0, 1.0, 0.0).astype(BF16)

    loads[1].wait()
    v_all = v[...].reshape(levels * rank, rows)
    v_perm = jnp.dot(v_all[: dev_bits * rank], one_hot[...], preferred_element_type=F32).astype(BF16)
    loads[2].wait()
    loads[3].wait()
    for copy in loads[4:]:
        copy.start()
    coef = jnp.dot(v_perm, src[...], preferred_element_type=F32)
    staged[...] = coef
    pl.semaphore_wait(barrier, len(partners))
    up_copies, low_copies = {}, {}
    for i in reversed(range(upper)):
        first = (upper - 1 - i) * rank
        for q in range(base):
            up_send[i, q] = staged[first + q * part:first + (q + 1) * part]
        for k in reversed(range(1, base)):
            up_copies[i, k] = send(up_send.at[i, flip(mine, k)], up_recv.at[i, k], k)
    chip_copies = {}
    bit = lax.rem(me, 2)
    for p in range(base_bits):
        first = (dev_bits - 1 - p) * rank
        size = rank >> p
        if p == 0:
            low_send[0][0] = staged[first:first + size]
            low_copies[1] = send(low_send[0].at[0], low_full[0].at[0], 1)
            continue
        for q in range(1 << p):
            low_send[p][q % 2, q // 2] = staged[first + q * size:first + (q + 1) * size]
        chip_copies[p] = send(low_send[p].at[1 - bit], low_chip[p], 1)

    for c in range(rows // 128):
        row = lax.broadcasted_iota(jnp.int32, (128, rows), 0).astype(F32) + c * 128.0
        one_hot_t[c * 128:(c + 1) * 128, :] = jnp.where(local == row, 1.0, 0.0).astype(BF16)
    chunk = rows // 4

    def order_rows(c):
        at = pl.ds(c * chunk, chunk)
        ordered[at, :] = jnp.dot(one_hot[at, :], src[...], preferred_element_type=F32).astype(BF16)

    order_rows(0)
    order_rows(1)

    for p in range(1, base_bits):
        chip_copies[p].wait_recv()
        low_sum[p][...] = low_send[p][bit] + low_chip[p][...]
        for k in reversed(range(1 << p, 2 << p, 2)):
            piece = lax.div(lax.rem(flip(mine, k), 1 << p), 2)
            low_copies[k] = send(low_sum[p].at[piece], low_recv[p].at[(k - (1 << p)) // 2], k)
    order_rows(2)
    order_rows(3)

    own_copies, above_copies, up_gather = {}, {}, {}

    def plane_sum(i):
        for k in reversed(range(1, base)):
            up_copies[i, k].wait_recv()
        total = up_send[i, mine]
        for k in range(1, base):
            total = total + up_recv[i, k]
        return total

    def send_group(g, i, value):
        start, bits = groups[g]
        at = i - (start - base_bits)
        hold[g - 1][at] = value
        if at < bits:
            for k in reversed(range(1 << at, 2 << at)):
                own_copies[g, k] = send(hold[g - 1].at[at], recv_own[g - 1].at[k], k << start)
        else:
            for k in reversed(range(1, 1 << bits)):
                above_copies[g, i, k] = send(
                    hold[g - 1].at[at], recv_above[g - 1].at[at - bits, k], k << start
                )

    def gather_level(g, j):
        i = groups[g][0] - base_bits + j
        total = None
        for k in range(1 << j, 2 << j):
            own_copies[g, k].wait_recv()
            total = recv_own[g - 1][k] if total is None else total + recv_own[g - 1][k]
        up_full[i, mine] = total
        for k in reversed(range(1, base)):
            up_gather[i, k] = send(up_full.at[i, mine], up_full.at[i, mine], k)

    for i in reversed(range(upper)):
        send_group(1, i, plane_sum(i))

    loads[4].wait()
    lane_all = lax.broadcasted_iota(jnp.int32, (1, dev_bits * rank), 1)
    keep = jnp.zeros((1, dev_bits * rank), F32)
    for l in range(dev_bits):
        inside = (lane_all >= l * rank) & (lane_all < l * rank + ranks_ref[l])
        keep = jnp.where(inside, 1.0, keep)
    loads[5].wait()
    u_all = u[...].reshape(levels * rank, rows)
    nt = (((1,), (1,)), ((), ()))
    for c in range(4):
        at = pl.ds(c * chunk, chunk)
        u_perm[at, :] = (
            lax.dot_general(one_hot_t[at, :], u_all[: dev_bits * rank], nt, preferred_element_type=F32) * keep
        ).astype(BF16)
    loads[6].wait()

    def mix():
        for c in range(4):
            at = pl.ds(c * chunk, chunk)
            for g in range(rows // leaf_size):
                cols = slice(g * leaf_size, (g + 1) * leaf_size)
                mixed[at, cols] = jnp.dot(
                    one_hot_t[at, cols], leaf[cols, :], preferred_element_type=F32
                ).astype(BF16)

    low_gather = []

    def low_levels():
        for copy in low_copies.values():
            copy.wait_recv()
        for p in range(1, base_bits):
            total = low_recv[p][0]
            for k in range(1, 1 << p - 1):
                total = total + low_recv[p][k]
            slot = lax.rem(mine, 1 << p)
            low_full[p][slot] = total
            for k in range(1, 1 << p):
                low_gather.append(send(low_full[p].at[slot], low_full[p].at[slot], k))

    def near_levels():
        near_at = 0
        for l in range(dev_bits, levels):
            cluster = rows >> l - dev_bits + 1
            for g in range(rows // cluster):
                for_u = slice(g * cluster, (g + 1) * cluster)
                sib = g ^ 1
                for_v = slice(sib * cluster, (sib + 1) * cluster)
                near[near_at:near_at + rank, :] = jnp.dot(
                    v_all[l * rank:(l + 1) * rank, for_v], ordered[for_v, :], preferred_element_type=F32
                ).astype(BF16)
                inside = lax.broadcasted_iota(jnp.int32, (1, rank), 1) < ranks_ref[l]
                u_near[:, near_at:near_at + rank] = (
                    lax.dot_general(
                        one_hot_t[:, for_u], u_all[l * rank:(l + 1) * rank, for_u], nt, preferred_element_type=F32
                    )
                    * jnp.where(inside, 1.0, 0.0)
                ).astype(BF16)
                near_at += rank

    def apply_rows(c):
        at = pl.ds(c * chunk, chunk)
        total = jnp.dot(mixed[at, :], ordered[...], preferred_element_type=F32)
        if levels > dev_bits:
            total = total + jnp.dot(u_near[at, :], near[...], preferred_element_type=F32)
        acc[at, :] = total

    fillers = [mix, low_levels, near_levels] + [functools.partial(apply_rows, c) for c in range(4)]
    fillers.pop(0)()
    for g in range(1, len(groups)):
        start, bits = groups[g]
        for i in reversed(range(start + bits - base_bits, upper)):
            total = hold[g - 1][i - (start - base_bits)]
            for k in reversed(range(1, 1 << bits)):
                above_copies[g, i, k].wait_recv()
                total = total + recv_above[g - 1][i - (start + bits - base_bits), k]
            send_group(g + 1, i, total)
        for j in range(bits):
            gather_level(g, j)
            if low_levels in fillers and j < bits - 1:
                fillers.pop(0)()
    for filler in fillers:
        filler()

    for copy in low_gather:
        copy.wait_recv()
    for p in range(base_bits):
        first = (dev_bits - 1 - p) * rank
        size = rank >> p
        for q in range(1 << p):
            staged[first + q * size:first + (q + 1) * size, :] = low_full[p][q]
    for i in range(upper):
        for k in range(1, base):
            up_gather[i, k].wait_recv()
        first = (dev_bits - 1 - (base_bits + i)) * rank
        for q in range(base):
            staged[first + q * part:first + (q + 1) * part, :] = up_full[i, q]
    far[...] = staged[...].astype(BF16)
    for copy in copies:
        copy.wait_send()


def finish(acc, u_perm, far, out_hbm, out, out_sem):
    chunk = acc.shape[0] // 8
    stores = []
    for c in range(8):
        at = pl.ds(c * chunk, chunk)
        total = acc[at, :] + jnp.dot(u_perm[at, :], far[...], preferred_element_type=F32)
        out[at, :] = total.astype(BF16)
        copy = pltpu.make_async_copy(out.at[at], out_hbm.at[at], out_sem.at[c])
        copy.start()
        stores.append(copy)
    for copy in stores:
        copy.wait()


def per_device(sources, tree_perm, leaf_blocks, u_factors, v_factors, level_ranks):
    rows, rhs = sources.shape
    leaf_size = leaf_blocks.shape[1]
    levels, rank, _ = u_factors.shape
    row_size, col_size = lax.axis_size("row"), lax.axis_size("col")
    dev_bits = (row_size * col_size).bit_length() - 1
    groups = split_bits(dev_bits)
    base_bits = groups[0][1]
    base = 1 << base_bits
    upper = dev_bits - base_bits
    part = rank // base
    cfg = (rows, rhs, leaf_size, levels, rank, row_size, col_size, groups)
    near_rows = rank * sum(2 << i for i in range(levels - dev_bits))
    vmem = pltpu.VMEM

    low = [vmem((1 << p, rank >> p, rhs), F32) for p in range(base_bits)]
    low_pairs = [vmem((1, rank, rhs), F32)] + [vmem((2, 1 << p - 1, rank >> p, rhs), F32) for p in range(1, base_bits)]
    low_half = [vmem((max(1 << p >> 1, 1), rank >> p, rhs), F32) for p in range(base_bits)]
    up = max(upper, 1)
    scratch = [
        vmem((rows, rhs), BF16),
        vmem(leaf_blocks.shape, BF16),
        vmem(u_factors.shape, BF16),
        vmem(v_factors.shape, BF16),
        vmem((rows, rows), BF16),
        vmem((rows, rows), BF16),
        vmem((rows, rhs), BF16),
        vmem((rows, rows), BF16),
        vmem((rows, max(near_rows, rank)), BF16),
        vmem((max(near_rows, rank), rhs), BF16),
        vmem((dev_bits * rank, rhs), F32),
    ]
    scratch += low_pairs + low_half + low + low_half + low_half
    scratch += [vmem((up, base, part, rhs), F32)] * 3
    scratch += [vmem((dev_bits - start, part, rhs), F32) for start, _ in groups[1:]]
    scratch += [vmem((1 << bits, part, rhs), F32) for _, bits in groups[1:]]
    scratch += [
        vmem((max(dev_bits - start - bits, 1), 1 << bits, part, rhs), F32) for start, bits in groups[1:]
    ]
    total = (2 * upper + 2) * base + sum((dev_bits - start) << bits for start, bits in groups[1:])
    scratch += [
        pltpu.SMEM(level_ranks.shape, jnp.int32),
        vmem((1, rows), jnp.int32),
        pltpu.SemaphoreType.DMA((7,)),
        pltpu.SemaphoreType.DMA((total,)),
        pltpu.SemaphoreType.DMA((total,)),
    ]
    wide = -(-dev_bits * rank // 128) * 128
    kept = rows * rhs * 4 + rows * wide * 2 + dev_bits * rank * rhs * 2
    any_space = pl.BlockSpec(memory_space=pl.ANY)
    vmem_space = pl.BlockSpec(memory_space=pltpu.VMEM)
    acc, u_perm, far = pl.pallas_call(
        functools.partial(kernel, cfg),
        out_shape=(
            pltpu.VMEM((rows, rhs), F32),
            pltpu.VMEM((rows, dev_bits * rank), BF16),
            pltpu.VMEM((dev_bits * rank, rhs), BF16),
        ),
        in_specs=[any_space] * 6,
        out_specs=(vmem_space, vmem_space, vmem_space),
        scratch_shapes=scratch,
        compiler_params=pltpu.CompilerParams(
            collective_id=0, has_side_effects=True, vmem_limit_bytes=VMEM_BYTES - kept - 96 * 1024
        ),
    )(level_ranks, tree_perm.reshape(1, rows), sources, leaf_blocks, u_factors, v_factors)
    return pl.pallas_call(
        finish,
        out_shape=jax.ShapeDtypeStruct((rows, rhs), BF16),
        in_specs=[vmem_space, vmem_space, vmem_space],
        out_specs=any_space,
        scratch_shapes=[vmem((rows, rhs), BF16), pltpu.SemaphoreType.DMA((8,))],
        compiler_params=pltpu.CompilerParams(vmem_limit_bytes=8 * 1024 * 1024),
    )(acc, u_perm, far)


def solution(mesh):
    placed = (
        P(("row", "col"), None),
        P(("row", "col")),
        P(("row", "col"), None),
        P(None, None, ("row", "col")),
        P(None, None, ("row", "col")),
        P(),
    )
    return jax.shard_map(
        per_device, mesh=mesh, in_specs=placed, out_specs=P(("row", "col"), None), check_vma=False
    )
```
